32 devices in a mesh: ep: 8 (over z, x), corner: 4 (over y, core).
Axes of the slice: x: 2, y: 2, z: 4, core: 2. Of those that a mesh axis runs over, the one named last changes fastest.
Arguments:
- required: float32 [8, 262144], P('corner', 'ep'), may hold values from -3 to 3
- arrival: float32 [8, 262144], P('corner', 'ep'), may hold values from -7.2 to 7.2
- hold_required: float32 [8, 262144], P('corner', 'ep'), may hold values from -5.4 to 5.4
- early_arrival: float32 [8, 262144], P('corner', 'ep'), may hold values from -3 to 3
- part_ids: int32 [262144], P('ep'), may hold values from 0 to 63
- bin_edges: int32 [512], replicated, may hold values from -4096 to -1, as said below
Outputs:
- part_hist: float32 [64, 8, 2, 512], P(None, 'corner')
- part_tns: float32 [64, 8, 2], P(None, 'corner')
- part_share: float32 [64], replicated
- tns: float32 [8, 2], P('corner')
- wns: float32 [8, 2], P('corner')
- worst: float32 [2, 262144], P(None, 'ep')
The draws below stay inside these ranges and needn't reach their ends.
Inputs may be any that keep to these rules, and one draw needn't show every extreme that they name: `bin_edges`: strictly increasing and negative; consecutive nodes differ by 1 to 8.
All inputs are finite; a program needn't handle non-finite values.
Results may differ from the reference program's by a relative error of at most 0.0003.
Values sent between devices are 32-bit elements; how exact they have to be, the bound alone decides.
A program may use at most 64 MiB of HBM per device.

```python
import math
import jax
import jax.numpy as jnp
import numpy as np
from jax import lax

BINS = 512
GROUPS = 64
CORNERS = 8
ENDPOINTS = 262144


def rising(key, scale):
    position = jnp.arange(ENDPOINTS, dtype=jnp.float32) / ENDPOINTS
    factor = 1.0 + 2.0 * position
    values = scale * factor * jax.random.normal(key, (CORNERS, ENDPOINTS), jnp.float32)
    return jnp.clip(values, -18.0 * scale, 18.0 * scale)


def draw_arrival(key, part):
    return rising(jax.random.fold_in(key, 11), 0.4)


def draw_hold_required(key, part):
    return rising(jax.random.fold_in(key, 23), 0.3)


def draw_bin_edges(key, part):
    gaps = jax.random.randint(jax.random.fold_in(key, 37), (BINS,), 1, 9, jnp.int32)
    return (-jnp.cumsum(gaps)[::-1]).astype(jnp.int32)


def with_ends(result, rng, low, largest):
    spot = [jax.random.randint(jax.random.fold_in(rng, axis), (), 0, length) for axis, length in enumerate(result.shape)]
    longest = result.shape.index(max(result.shape))
    neighbour = spot[:longest] + [(spot[longest] + 1) % result.shape[longest]] + spot[longest + 1:]
    return result.at[tuple(spot)].set(low).at[tuple(neighbour)].set(largest)


def shard_levels(stream_key, dims, shards, least, top_value):
    loudness, own = 1.0, jax.random.fold_in(stream_key, 6)
    for dim, blocks in shards:
        steps = jnp.exp(jax.random.uniform(jax.random.fold_in(own, dim), (blocks,), jnp.float32, least / len(shards), top_value / len(shards)))
        loudness = loudness * jnp.repeat(steps, dims[dim] // blocks).reshape([-1 if axis == dim else 1 for axis in range(len(dims))])
    return loudness


def rank_bounds(amount, lean):
    weights = [(1 << 20) // math.isqrt(rank ** lean) + 1 for rank in range(1, amount + 1)]
    deviation = 1 + sum(weights) // (1 << 30)
    return np.cumsum(np.array([max(1, weight // deviation) for weight in weights]))


def ranked(own_key, dims, count, slope):
    listing = rank_bounds(count, slope)
    ticket = jax.random.randint(jax.random.fold_in(own_key, 1), dims, 0, int(listing[count - 1]))
    rank = jnp.searchsorted(jnp.asarray(listing, jnp.int32), ticket, side="right")
    return jax.random.permutation(jax.random.fold_in(own_key, 2), count)[rank].astype(jnp.int32)


def centred(stream_key, dims, deviation, limit, pieces=(), kind=jnp.bfloat16):
    level = shard_levels(stream_key, dims, pieces, -0.22, 0.18) if pieces else 1.0
    entries = jax.random.normal(stream_key, dims, jnp.float32) * deviation * level
    return jnp.minimum(jnp.maximum(entries, -limit), limit).astype(kind)


def setup_inputs(seed: int = 0) -> dict:
    splits = jax.random.split(jax.random.key(seed), 7)
    required = centred(splits[0], (CORNERS, ENDPOINTS), 0.5, 3.0, ((0, 4), (1, 8)), jnp.float32)
    arrival = draw_arrival(jax.random.fold_in(splits[6], 71), 0)
    hold_required = draw_hold_required(jax.random.fold_in(splits[6], 71), 0)
    early_arrival = centred(splits[3], (CORNERS, ENDPOINTS), 0.5, 3.0, ((0, 4), (1, 8)), jnp.float32)
    part_ids = with_ends(ranked(splits[4], (ENDPOINTS,), GROUPS, 1), jax.random.fold_in(splits[4], 3), 0, GROUPS - 1).astype(jnp.int32)
    bin_edges = draw_bin_edges(jax.random.fold_in(splits[6], 71), 0)
    return dict(required=required, arrival=arrival, hold_required=hold_required, early_arrival=early_arrival, part_ids=part_ids, bin_edges=bin_edges)


def node_tables(bin_edges):
    nodes = bin_edges.astype(jnp.float32) * 0.001
    upper = jnp.concatenate([nodes[1:], jnp.zeros((1,), jnp.float32)])
    lower = jnp.concatenate([nodes[:1] - 1.0, nodes[:-1]])
    return nodes, lower, upper


def weights_at(index, level, nodes, lower, upper):
    node = nodes[index]
    low = lower[index]
    high = upper[index]
    rise = (level - low) / (node - low)
    fall = (high - level) / (high - node)
    return jnp.maximum(jnp.minimum(rise, fall), 0.0)


def rounded(values):
    narrow = lax.optimization_barrier(values.astype(jnp.bfloat16))
    return narrow.astype(jnp.float32)


def histogram(slack, part_ids, nodes, lower, upper):
    level = jnp.clip(slack, nodes[0], 0.0)
    first = jnp.searchsorted(nodes, level, side="right").astype(jnp.int32) - 1
    first = jnp.clip(first, 0, BINS - 1).astype(jnp.int32)
    second = jnp.minimum(first + 1, BINS - 1).astype(jnp.int32)
    w_first = rounded(weights_at(first, level, nodes, lower, upper))
    w_second = rounded(jnp.where(first + 1 < BINS, weights_at(second, level, nodes, lower, upper), 0.0))
    total = jax.ops.segment_sum(w_first, part_ids * BINS + first, num_segments=GROUPS * BINS)
    total = total + jax.ops.segment_sum(w_second, part_ids * BINS + second, num_segments=GROUPS * BINS)
    return total.reshape(GROUPS, BINS)


def reference(required, arrival, hold_required, early_arrival, part_ids, bin_edges):
    nodes, lower, upper = node_tables(bin_edges)
    setup = required - arrival
    hold = early_arrival - hold_required

    def one_corner(pair):
        return jnp.stack([histogram(pair[0], part_ids, nodes, lower, upper), histogram(pair[1], part_ids, nodes, lower, upper)], axis=1)

    hists = lax.map(one_corner, (setup, hold))
    density = GROUPS * BINS / ENDPOINTS
    part_hist = jnp.transpose(hists, (1, 0, 2, 3)) * density
    neg_setup = jnp.minimum(setup, 0.0)
    neg_hold = jnp.minimum(hold, 0.0)
    share = GROUPS / ENDPOINTS
    part_setup = jax.ops.segment_sum(neg_setup.T, part_ids, num_segments=GROUPS)
    part_holdn = jax.ops.segment_sum(neg_hold.T, part_ids, num_segments=GROUPS)
    part_tns = jnp.stack([part_setup, part_holdn], axis=2) * share
    counts = jax.ops.segment_sum(jnp.ones(part_ids.shape, jnp.float32), part_ids, num_segments=GROUPS)
    part_share = counts * share
    tns = jnp.stack([jnp.sum(neg_setup, axis=1), jnp.sum(neg_hold, axis=1)], axis=1) * (1.0 / ENDPOINTS)
    wns = jnp.stack([jnp.min(setup, axis=1), jnp.min(hold, axis=1)], axis=1)
    worst = jnp.stack([jnp.min(setup, axis=0), jnp.min(hold, axis=0)], axis=0)
    return (part_hist, part_tns, part_share, tns, wns, worst)
```

```python
import functools
import jax
import jax.numpy as jnp
from jax import lax
from jax.experimental import pallas as pl
from jax.experimental.pallas import tpu as pltpu
from jax.sharding import PartitionSpec as P

GROUPS = 64
HIGH = 4
LANES = 128
EXTRA = 16
HALF = 512
MESH = pl.DeviceIdType.MESH


def pick(table, index):
    return jnp.take_along_axis(table, index, axis=1, mode="promise_in_bounds")


def make_tables(edges_ref):
    nodes = edges_ref[...].astype(jnp.float32) * 0.001
    lane = lax.broadcasted_iota(jnp.int32, (8, LANES), 1)
    rows = [jnp.broadcast_to(nodes[q : q + 1], (8, LANES)) for q in range(4)]
    third = []
    for j in range(8):
        index = (8 * lane + j) & 127
        parts = [pick(row, index) for row in rows]
        value = parts[3]
        for q in (2, 1, 0):
            value = jnp.where(lane < 16 * (q + 1), parts[q], value)
        third.append(value)
    following = pick(third[0], jnp.minimum(lane + 1, LANES - 1))
    third.append(jnp.where(lane >= 63, 0.0, following))
    second = [pick(third[0], (8 * lane + j) & 63) for j in range(1, 8)]
    first = [pick(third[0], jnp.full((8, LANES), 8 * i, jnp.int32)) for i in range(1, 8)]
    lowest = pick(third[0], jnp.zeros((8, LANES), jnp.int32))
    return first, second, third, lowest


def search(tables, slack):
    first, second, third, lowest = tables
    level = jnp.minimum(jnp.maximum(slack, lowest), 0.0)
    group = jnp.zeros(level.shape, jnp.int32)
    for bound in first:
        group += (level >= bound).astype(jnp.int32)
    finer = group * 8
    for table in second:
        finer += (level >= pick(table, group)).astype(jnp.int32)
    index = finer * 8
    low = pick(third[0], finer)
    high = pick(third[8], finer)
    inner = [pick(table, finer) for table in third[1:8]]
    for value in inner:
        above = level >= value
        index += above.astype(jnp.int32)
        low = jnp.where(above, value, low)
    for value in reversed(inner):
        high = jnp.where(level < value, value, high)
    scale = 1.0 / (high - low)
    return index, (high - level) * scale, (level - low) * scale


def compute_kernel(req, arr, hreq, early, ids, edges, hist_out, stats_out, worst_out, acc, least):
    corners, rows = req.shape
    combos = 2 * corners
    halves = 8 // combos
    depth = halves * HALF
    tables = make_tables(edges)
    acc[...] = jnp.zeros_like(acc)
    least[...] = jnp.full_like(least, jnp.inf)
    narrow = jnp.bfloat16
    iota = lax.broadcasted_iota(jnp.int32, (16, depth), 0)
    iota_low = iota.astype(jnp.float32).astype(narrow)
    zero = jnp.zeros((16, depth), narrow)
    one = jnp.ones((16, depth), narrow)

    def block(step, carry):
        slabs, parts = [], []
        for half in range(halves):
            at = pl.ds(pl.multiple_of(step * depth + half * HALF, HALF), HALF)
            setup = req[:, at] - arr[:, at]
            hold = early[:, at] - hreq[:, at]
            worst_out[0:1, at] = jnp.min(setup, axis=0, keepdims=True)
            worst_out[1:2, at] = jnp.min(hold, axis=0, keepdims=True)
            slabs += [setup, hold]
            parts.append(jnp.broadcast_to(ids[:, at], (combos, HALF)))
        slab = jnp.concatenate(slabs, axis=0)
        part = jnp.concatenate(parts, axis=0)
        low_at, code, w_first, w_second = [], [], [], []
        smallest = least[...]
        for lane in range(0, HALF, LANES):
            piece = slab[:, lane : lane + LANES]
            smallest = jnp.minimum(smallest, piece)
            index, wa, wb = search(tables, piece)
            low_at.append((index & (LANES - 1)).astype(jnp.float32))
            code.append(((index >> 7) * GROUPS + part[:, lane : lane + LANES]).astype(jnp.float32))
            w_first.append(wa)
            w_second.append(wb)
        least[...] = smallest
        low_at, code, w_first, w_second = (
            jnp.concatenate(v, axis=1) for v in (low_at, code, w_first, w_second)
        )
        neg = jnp.minimum(slab, 0.0)
        piece_a = neg.astype(narrow).astype(jnp.float32)
        rest = neg - piece_a
        piece_b = rest.astype(narrow).astype(jnp.float32)
        piece_c = rest - piece_b
        for r in range(combos):

            def spread(v):
                row = jnp.concatenate(
                    [v[r + combos * h : r + combos * h + 1] for h in range(halves)], axis=1
                )
                return jnp.broadcast_to(row, (16, depth)).astype(narrow)

            at_low, at_code, wa, wb = (spread(v) for v in (low_at, code, w_first, w_second))
            left = []
            for start in range(0, LANES, 16):
                row = iota_low + narrow(start)
                next_row = iota_low + narrow(start - 1)
                left.append(
                    jnp.where(at_low == row, wa, jnp.where(at_low == next_row, wb, zero))
                )
            tail = jnp.where(at_low == narrow(LANES - 1), wb, zero)
            tail = jnp.where(iota_low == narrow(0), tail, zero)
            for place, v in ((1, piece_a), (2, piece_b), (3, piece_c)):
                tail = jnp.where(iota_low == narrow(place), spread(v), tail)
            tail = jnp.where(iota_low == narrow(4), one, tail)
            left.append(tail)
            left = jnp.concatenate(left, axis=0)
            right = jnp.concatenate(
                [
                    jnp.where(at_code == iota_low + narrow(start), one, zero)
                    for start in range(0, HIGH * GROUPS, 16)
                ],
                axis=0,
            )
            acc[r] += lax.dot_general(
                left, right, (((1,), (1,)), ((), ())), preferred_element_type=jnp.float32
            )
        return carry

    lax.fori_loop(0, rows // depth, block, 0)

    lane = lax.broadcasted_iota(jnp.int32, (1, HIGH * GROUPS), 1)
    stats_out[...] = jnp.zeros_like(stats_out)

    def fold(v):
        v = v[:, :LANES] + v[:, LANES:]
        return v + pltpu.roll(jnp.broadcast_to(v, (8, LANES)), GROUPS, 1)[0:1]

    for r in range(combos):
        over = jnp.broadcast_to(acc[r, LANES : LANES + 1], (8, HIGH * GROUPS))
        over = pltpu.roll(over, GROUPS, 1)[0:1]
        acc[r, 0:1] += jnp.where(lane >= GROUPS, over, 0.0)
        turned = acc[r, 0:LANES].T
        for g in range(HIGH):
            hist_out[r * GROUPS : (r + 1) * GROUPS, g * LANES : (g + 1) * LANES] = turned[
                g * GROUPS : (g + 1) * GROUPS
            ]
        total = (
            acc[r, LANES + 1 : LANES + 2]
            + acc[r, LANES + 2 : LANES + 3]
            + acc[r, LANES + 3 : LANES + 4]
        )
        stats_out[r : r + 1] = fold(total)
    stats_out[combos : combos + 1] = fold(acc[0, LANES + 4 : LANES + 5])
    stats_out[8:16] = jnp.broadcast_to(jnp.min(least[...], axis=1, keepdims=True), (8, LANES))


def exchange_kernel(
    n, nc, density,
    hist, stats, worst, hist_out, stats_out, worst_out,
    hist_in, stats_in, worst_in,
    hs, hr, gs, gr, ss, sr, ws, wr, vs, vr,
):
    me = lax.axis_index("ep")
    mc = lax.axis_index("corner")
    chunk = hist.shape[0] // n
    width = worst.shape[1] // nc
    barrier = pltpu.get_barrier_semaphore()
    for d in range(1, n):
        pl.semaphore_signal(
            barrier, inc=1, device_id={"ep": lax.rem(me + d, n)}, device_id_type=MESH
        )
    for d in range(1, nc):
        pl.semaphore_signal(
            barrier, inc=1, device_id={"corner": lax.rem(mc + d, nc)}, device_id_type=MESH
        )
    pl.semaphore_wait(barrier, n - 1 + nc - 1)

    def send(src, dst, s_sem, r_sem, target):
        copy = pltpu.make_async_remote_copy(
            src_ref=src, dst_ref=dst, send_sem=s_sem, recv_sem=r_sem,
            device_id=target, device_id_type=MESH,
        )
        copy.start()
        return copy

    def lanes(k):
        return pl.ds(pl.multiple_of(k * width, LANES), width)

    def rows(k):
        return pl.ds(pl.multiple_of(k * chunk, 8), chunk)

    scatter, shares, mins = [], [], []
    for d in range(1, nc):
        t = lax.rem(mc + d, nc)
        mins.append(
            send(worst.at[:, lanes(t)], worst_in.at[d], ws.at[d], wr.at[d], {"corner": t})
        )
    for d in range(1, n):
        t = lax.rem(me + d, n)
        scatter.append(send(hist.at[rows(t)], hist_in.at[d], hs.at[d], hr.at[d], {"ep": t}))
    for d in range(1, n):
        t = lax.rem(me + d, n)
        shares.append(send(stats, stats_in.at[me], ss.at[d], sr.at[d], {"ep": t}))

    for copy in mins:
        copy.wait_recv()
    low = worst[:, lanes(mc)]
    for d in range(1, nc):
        low = jnp.minimum(low, worst_in[d])
    worst_out[:, lanes(mc)] = low
    spread = []
    for d in range(1, nc):
        t = lax.rem(mc + d, nc)
        part = worst_out.at[:, lanes(mc)]
        spread.append(send(part, part, vs.at[d], vr.at[d], {"corner": t}))

    total = hist[rows(me)]
    for d in range(1, n):
        scatter[d - 1].wait_recv()
        total += hist_in[d]
    hist_out[rows(me)] = total * density
    gather = []
    for d in range(1, n):
        t = lax.rem(me + d, n)
        part = hist_out.at[rows(me)]
        gather.append(send(part, part, gs.at[d], gr.at[d], {"ep": t}))

    for copy in shares:
        copy.wait_recv()
    stats_in[me] = stats[...]
    added = stats_in[0, 0:8]
    least = stats_in[0, 8:16]
    for k in range(1, n):
        added += stats_in[k, 0:8]
        least = jnp.minimum(least, stats_in[k, 8:16])
    stats_out[0:8] = added
    stats_out[8:16] = least
    for copy in spread + gather:
        copy.wait_recv()
    for copy in mins + scatter + shares + spread + gather:
        copy.wait_send()


def on_device(required, arrival, hold_required, early_arrival, part_ids, bin_edges):
    corners, rows = required.shape
    n, nc = lax.axis_size("ep"), lax.axis_size("corner")
    endpoints = rows * n
    bins = bin_edges.shape[0]
    combos = 2 * corners
    f32 = jnp.float32
    vmem = pl.BlockSpec(memory_space=pltpu.VMEM)
    shapes = (
        jax.ShapeDtypeStruct((combos * GROUPS, bins), f32),
        jax.ShapeDtypeStruct((16, LANES), f32),
        jax.ShapeDtypeStruct((2, rows), f32),
    )
    hist, stats, worst = pl.pallas_call(
        compute_kernel,
        out_shape=shapes,
        in_specs=[vmem] * 6,
        out_specs=[vmem] * 3,
        scratch_shapes=[
            pltpu.VMEM((combos, LANES + EXTRA, HIGH * GROUPS), f32),
            pltpu.VMEM((8, LANES), f32),
        ],
        name="local_report",
    )(
        required, arrival, hold_required, early_arrival,
        part_ids.reshape(1, rows), bin_edges.reshape(bins // LANES, LANES),
    )
    dma = pltpu.SemaphoreType.DMA
    hist, stats, worst = pl.pallas_call(
        functools.partial(exchange_kernel, n, nc, GROUPS * bins / endpoints),
        out_shape=shapes,
        in_specs=[vmem] * 3,
        out_specs=[vmem] * 3,
        scratch_shapes=[
            pltpu.VMEM((n, combos * GROUPS // n, bins), f32),
            pltpu.VMEM((n, 16, LANES), f32),
            pltpu.VMEM((nc, 2, rows // nc), f32),
        ]
        + [dma((n,))] * 6
        + [dma((nc,))] * 4,
        compiler_params=pltpu.CompilerParams(collective_id=0, has_side_effects=True),
        name="exchange",
    )(hist, stats, worst)
    part_hist = hist.reshape(2, corners, GROUPS, bins).transpose(2, 1, 0, 3)
    share = GROUPS / endpoints
    sums = stats[:combos, :GROUPS].reshape(2, corners, GROUPS)
    part_tns = sums.transpose(2, 1, 0) * share
    part_share = stats[combos, :GROUPS] * share
    tns = jnp.sum(sums, axis=2).T * (1.0 / endpoints)
    least = jnp.min(stats[8:16, 0].reshape(8 // combos, 2, corners), axis=0)
    return (part_hist, part_tns, part_share, tns, least.T, worst)


def solution(mesh):
    in_specs = (
        P("corner", "ep"),
        P("corner", "ep"),
        P("corner", "ep"),
        P("corner", "ep"),
        P("ep"),
        P(),
    )
    out_specs = (
        P(None, "corner", None, None),
        P(None, "corner", None),
        P(),
        P("corner", None),
        P("corner", None),
        P(None, "ep"),
    )
    return jax.shard_map(
        on_device, mesh=mesh, in_specs=in_specs, out_specs=out_specs, check_vma=False
    )
```

```python
import functools
import jax
import jax.numpy as jnp
from jax import lax
from jax.experimental import pallas as pl
from jax.experimental.pallas import tpu as pltpu
from jax.sharding import PartitionSpec as P

GROUPS = 64
HIGH = 4
LANES = 128
EXTRA = 16
HALF = 1024
DEPTH = 4096
MESH = pl.DeviceIdType.MESH


def pick(table, index):
    return jnp.take_along_axis(table, index, axis=1, mode="promise_in_bounds")


def make_tables(edges_ref):
    nodes = edges_ref[...].astype(jnp.float32) * 0.001
    lane = lax.broadcasted_iota(jnp.int32, (8, LANES), 1)
    rows = [jnp.broadcast_to(nodes[q : q + 1], (8, LANES)) for q in range(4)]
    third = []
    for j in range(8):
        index = (8 * lane + j) & 127
        parts = [pick(row, index) for row in rows]
        value = parts[3]
        for q in (2, 1, 0):
            value = jnp.where(lane < 16 * (q + 1), parts[q], value)
        third.append(value)
    following = pick(third[0], jnp.minimum(lane + 1, LANES - 1))
    third.append(jnp.where(lane >= 63, 0.0, following))
    second = [pick(third[0], (8 * lane + j) & 63) for j in range(1, 8)]
    first = [pick(third[0], jnp.full((8, LANES), 8 * i, jnp.int32)) for i in range(1, 8)]
    lowest = pick(third[0], jnp.zeros((8, LANES), jnp.int32))
    return first, second, third, lowest


def search(tables, slack):
    first, second, third, lowest = tables
    level = jnp.minimum(jnp.maximum(slack, lowest), 0.0)
    group = jnp.zeros(level.shape, jnp.int32)
    for bound in first:
        group += (level >= bound).astype(jnp.int32)
    finer = group * 8
    for table in second:
        finer += (level >= pick(table, group)).astype(jnp.int32)
    index = finer * 8
    low = pick(third[0], finer)
    high = pick(third[8], finer)
    inner = [pick(table, finer) for table in third[1:8]]
    for value in inner:
        above = level >= value
        index += above.astype(jnp.int32)
        low = jnp.where(above, value, low)
    for value in reversed(inner):
        high = jnp.where(level < value, value, high)
    scale = 1.0 / (high - low)
    return index, (high - level) * scale, (level - low) * scale


def search_kernel(req, arr, hreq, early, ids, edges, marks_out, worst_out, least_out):
    corners, rows = req.shape
    combos = 2 * corners
    halves = 8 // combos
    depth = halves * HALF
    tables = make_tables(edges)

    def block(step, smallest):
        slabs, parts, spans = [], [], []
        for half in range(halves):
            at = pl.ds(pl.multiple_of(step * depth + half * HALF, HALF), HALF)
            setup = req[:, at] - arr[:, at]
            hold = early[:, at] - hreq[:, at]
            worst_out[0:1, at] = jnp.min(setup, axis=0, keepdims=True)
            worst_out[1:2, at] = jnp.min(hold, axis=0, keepdims=True)
            slabs += [setup, hold]
            parts.append(jnp.broadcast_to(ids[:, at], (combos, HALF)))
            spans.append(at)
        slab = jnp.concatenate(slabs, axis=0)
        part = jnp.concatenate(parts, axis=0)
        low_at, code, w_first, w_second = [], [], [], []
        for lane in range(0, HALF, LANES):
            piece = slab[:, lane : lane + LANES]
            smallest = jnp.minimum(smallest, piece)
            index, wa, wb = search(tables, piece)
            low_at.append((index & (LANES - 1)).astype(jnp.float32))
            code.append(((index >> 7) * GROUPS + part[:, lane : lane + LANES]).astype(jnp.float32))
            w_first.append(wa)
            w_second.append(wb)
        marks = [jnp.concatenate(v, axis=1) for v in (low_at, code, w_first, w_second)]
        marks.append(jnp.minimum(slab, 0.0))
        for q, v in enumerate(marks):
            for half in range(halves):
                marks_out[q, :, spans[half]] = v[half * combos : (half + 1) * combos]
        return smallest

    start = jnp.full((8, LANES), jnp.inf, jnp.float32)
    smallest = lax.fori_loop(0, rows // depth, block, start)
    least_out[...] = jnp.broadcast_to(jnp.min(smallest, axis=1, keepdims=True), (8, LANES))


def report_kernel(
    n, nc, density,
    marks, worst, least, hist_out, stats_out, worst_out,
    acc, hist, hist_in, stats, stats_in, worst_in,
    hs, hr, gs, gr, ss, sr, ws, wr, vs, vr,
):
    combos, rows = marks.shape[1:]
    me = lax.axis_index("ep")
    mc = lax.axis_index("corner")
    chunk = GROUPS // n
    width = worst.shape[1] // nc
    narrow = jnp.bfloat16
    barrier = pltpu.get_barrier_semaphore()
    for d in range(1, n):
        pl.semaphore_signal(
            barrier, inc=1, device_id={"ep": lax.rem(me + d, n)}, device_id_type=MESH
        )
    for d in range(1, nc):
        pl.semaphore_signal(
            barrier, inc=1, device_id={"corner": lax.rem(mc + d, nc)}, device_id_type=MESH
        )
    pl.semaphore_wait(barrier, n - 1 + nc - 1)

    def send(src, dst, s_sem, r_sem, target):
        copy = pltpu.make_async_remote_copy(
            src_ref=src, dst_ref=dst, send_sem=s_sem, recv_sem=r_sem,
            device_id=target, device_id_type=MESH,
        )
        copy.start()
        return copy

    def lanes(k):
        return pl.ds(pl.multiple_of(k * width, LANES), width)

    mins = []
    for d in range(1, nc):
        t = lax.rem(mc + d, nc)
        mins.append(
            send(worst.at[:, lanes(t)], worst_in.at[d], ws.at[d], wr.at[d], {"corner": t})
        )

    iota_low = lax.broadcasted_iota(jnp.int32, (16, DEPTH), 0).astype(jnp.float32).astype(narrow)
    zero = jnp.zeros((16, DEPTH), narrow)
    one = jnp.ones((16, DEPTH), narrow)

    def product(r, first, last):
        def block(step, carry):
            at = pl.ds(pl.multiple_of(step * DEPTH, DEPTH), DEPTH)

            def row(q):
                return marks[q, r : r + 1, at]

            def spread(v):
                return jnp.broadcast_to(v, (16, DEPTH)).astype(narrow)

            at_low, at_code, wa, wb = (spread(row(q)) for q in range(4))
            neg = row(4)
            piece_a = neg.astype(narrow).astype(jnp.float32)
            rest = neg - piece_a
            piece_b = rest.astype(narrow).astype(jnp.float32)
            piece_c = rest - piece_b
            left = []
            for start in range(0, LANES, 16):
                left.append(
                    jnp.where(
                        at_low == iota_low + narrow(start),
                        wa,
                        jnp.where(at_low == iota_low + narrow(start - 1), wb, zero),
                    )
                )
            tail = jnp.where(at_low == narrow(LANES - 1), wb, zero)
            tail = jnp.where(iota_low == narrow(0), tail, zero)
            for place, v in ((1, piece_a), (2, piece_b), (3, piece_c)):
                tail = jnp.where(iota_low == narrow(place), spread(v), tail)
            left.append(jnp.where(iota_low == narrow(4), one, tail))
            right = [
                jnp.where(at_code == iota_low + narrow(start), one, zero)
                for start in range(0, HIGH * GROUPS, 16)
            ]
            acc[...] += lax.dot_general(
                jnp.concatenate(left, axis=0),
                jnp.concatenate(right, axis=0),
                (((1,), (1,)), ((), ())),
                preferred_element_type=jnp.float32,
            )
            return carry

        lax.fori_loop(first, last, block, 0)

    lane = lax.broadcasted_iota(jnp.int32, (1, HIGH * GROUPS), 1)

    def fold(v):
        v = v[:, :LANES] + v[:, LANES:]
        return v + pltpu.roll(jnp.broadcast_to(v, (8, LANES)), GROUPS, 1)[0:1]

    def settle(r):
        full = acc[...]
        over = jnp.broadcast_to(full[LANES : LANES + 1], (8, HIGH * GROUPS))
        over = pltpu.roll(over, GROUPS, 1)[0:1]
        acc[0:1] = full[0:1] + jnp.where(lane >= GROUPS, over, 0.0)
        turned = acc[0:LANES].T
        for k in range(n):
            for g in range(HIGH):
                top = g * GROUPS + k * chunk
                hist[r, k, :, g * LANES : (g + 1) * LANES] = turned[top : top + chunk]
        pieces = [full[LANES + 1 + i : LANES + 2 + i] for i in range(3)]
        stats[r : r + 1] = fold(pieces[0] + pieces[1] + pieces[2])
        if r == 0:
            stats[combos : combos + 1] = fold(full[LANES + 4 : LANES + 5])

    def scatter(r):
        copies = []
        for d in range(1, n):
            t = lax.rem(me + d, n)
            copies.append(
                send(hist.at[r, t], hist_in.at[r, d], hs.at[r, d], hr.at[r, d], {"ep": t})
            )
        return copies

    def gather(r, scattered):
        total = hist[r, me]
        for d in range(1, n):
            scattered[d - 1].wait_recv()
            total += hist_in[r, d]
        hist_out[r, me] = total * density
        copies = []
        for d in range(1, n):
            t = lax.rem(me + d, n)
            part = hist_out.at[r, me]
            copies.append(send(part, part, gs.at[r, d], gr.at[r, d], {"ep": t}))
        return copies

    steps = rows // DEPTH
    stats[...] = jnp.zeros_like(stats)
    stats[8:16] = least[...]
    sent, spread_out, gathered = [], [], []
    for r in range(combos):
        acc[...] = jnp.zeros_like(acc)
        product(r, 0, steps // 2)
        if r == 0:
            for copy in mins:
                copy.wait_recv()
            low = worst[:, lanes(mc)]
            for d in range(1, nc):
                low = jnp.minimum(low, worst_in[d])
            worst_out[:, lanes(mc)] = low
            for d in range(1, nc):
                t = lax.rem(mc + d, nc)
                part = worst_out.at[:, lanes(mc)]
                spread_out.append(send(part, part, vs.at[d], vr.at[d], {"corner": t}))
        else:
            gathered += gather(r - 1, sent[-1])
        product(r, steps // 2, steps)
        settle(r)
        sent.append(scatter(r))
    shares = []
    for d in range(1, n):
        t = lax.rem(me + d, n)
        shares.append(send(stats, stats_in.at[me], ss.at[d], sr.at[d], {"ep": t}))
    gathered += gather(combos - 1, sent[-1])
    for copy in shares:
        copy.wait_recv()
    stats_in[me] = stats[...]
    added = stats_in[0, 0:8]
    lowest = stats_in[0, 8:16]
    for k in range(1, n):
        added += stats_in[k, 0:8]
        lowest = jnp.minimum(lowest, stats_in[k, 8:16])
    stats_out[0:8] = added
    stats_out[8:16] = lowest
    for copy in spread_out + gathered:
        copy.wait_recv()
    for copy in mins + sum(sent, []) + shares + spread_out + gathered:
        copy.wait_send()


def on_device(required, arrival, hold_required, early_arrival, part_ids, bin_edges):
    corners, rows = required.shape
    n, nc = lax.axis_size("ep"), lax.axis_size("corner")
    endpoints = rows * n
    bins = bin_edges.shape[0]
    combos = 2 * corners
    f32 = jnp.float32
    vmem = pl.BlockSpec(memory_space=pltpu.VMEM)
    marks, worst, least = pl.pallas_call(
        search_kernel,
        out_shape=(
            jax.ShapeDtypeStruct((5, combos, rows), f32),
            jax.ShapeDtypeStruct((2, rows), f32),
            jax.ShapeDtypeStruct((8, LANES), f32),
        ),
        in_specs=[vmem] * 6,
        out_specs=[vmem] * 3,
        name="node_search",
    )(
        required, arrival, hold_required, early_arrival,
        part_ids.reshape(1, rows), bin_edges.reshape(bins // LANES, LANES),
    )
    dma = pltpu.SemaphoreType.DMA
    blocks = (combos, n, GROUPS // n, bins)
    hist, stats, worst = pl.pallas_call(
        functools.partial(report_kernel, n, nc, GROUPS * bins / endpoints),
        out_shape=(
            jax.ShapeDtypeStruct(blocks, f32),
            jax.ShapeDtypeStruct((16, LANES), f32),
            jax.ShapeDtypeStruct((2, rows), f32),
        ),
        in_specs=[vmem] * 3,
        out_specs=[vmem] * 3,
        scratch_shapes=[
            pltpu.VMEM((LANES + EXTRA, HIGH * GROUPS), f32),
            pltpu.VMEM(blocks, f32),
            pltpu.VMEM(blocks, f32),
            pltpu.VMEM((16, LANES), f32),
            pltpu.VMEM((n, 16, LANES), f32),
            pltpu.VMEM((nc, 2, rows // nc), f32),
        ]
        + [dma((combos, n))] * 4
        + [dma((n,))] * 2
        + [dma((nc,))] * 4,
        compiler_params=pltpu.CompilerParams(collective_id=0, has_side_effects=True),
        name="report",
    )(marks, worst, least)
    part_hist = hist.reshape(2, corners, GROUPS, bins).transpose(2, 1, 0, 3)
    share = GROUPS / endpoints
    sums = stats[:combos, :GROUPS].reshape(2, corners, GROUPS)
    part_tns = sums.transpose(2, 1, 0) * share
    part_share = stats[combos, :GROUPS] * share
    tns = jnp.sum(sums, axis=2).T * (1.0 / endpoints)
    least = jnp.min(stats[8:16, 0].reshape(8 // combos, 2, corners), axis=0)
    return (part_hist, part_tns, part_share, tns, least.T, worst)


def solution(mesh):
    in_specs = (
        P("corner", "ep"),
        P("corner", "ep"),
        P("corner", "ep"),
        P("corner", "ep"),
        P("ep"),
        P(),
    )
    out_specs = (
        P(None, "corner", None, None),
        P(None, "corner", None),
        P(),
        P("corner", None),
        P("corner", None),
        P(None, "ep"),
    )
    return jax.shard_map(
        on_device, mesh=mesh, in_specs=in_specs, out_specs=out_specs, check_vma=False
    )
```

```python
import functools
import jax
import jax.numpy as jnp
from jax import lax
from jax.experimental import pallas as pl
from jax.experimental.pallas import tpu as pltpu
from jax.sharding import PartitionSpec as P

GROUPS = 64
HIGH = 4
LANES = 128
EXTRA = 16
HALF = 1024
DEPTH = 4096
MESH = pl.DeviceIdType.MESH


def pick(table, index):
    return jnp.take_along_axis(table, index, axis=1, mode="promise_in_bounds")


def make_tables(edges_ref):
    nodes = edges_ref[...].astype(jnp.float32) * 0.001
    lane = lax.broadcasted_iota(jnp.int32, (8, LANES), 1)
    rows = [jnp.broadcast_to(nodes[q : q + 1], (8, LANES)) for q in range(4)]
    third = []
    for j in range(8):
        index = (8 * lane + j) & 127
        parts = [pick(row, index) for row in rows]
        value = parts[3]
        for q in (2, 1, 0):
            value = jnp.where(lane < 16 * (q + 1), parts[q], value)
        third.append(value)
    following = pick(third[0], jnp.minimum(lane + 1, LANES - 1))
    third.append(jnp.where(lane >= 63, 0.0, following))
    second = [pick(third[0], (8 * lane + j) & 63) for j in range(1, 8)]
    first = [pick(third[0], jnp.full((8, LANES), 8 * i, jnp.int32)) for i in range(1, 8)]
    lowest = pick(third[0], jnp.zeros((8, LANES), jnp.int32))
    return first, second, third, lowest


def search(tables, slack):
    first, second, third, lowest = tables
    level = jnp.minimum(jnp.maximum(slack, lowest), 0.0)
    group = jnp.zeros(level.shape, jnp.int32)
    for bound in first:
        group += (level >= bound).astype(jnp.int32)
    finer = group * 8
    for table in second:
        finer += (level >= pick(table, group)).astype(jnp.int32)
    index = finer * 8
    low = pick(third[0], finer)
    high = pick(third[8], finer)
    inner = [pick(table, finer) for table in third[1:8]]
    for value in inner:
        above = level >= value
        index += above.astype(jnp.int32)
        low = jnp.where(above, value, low)
    for value in reversed(inner):
        high = jnp.where(level < value, value, high)
    scale = 1.0 / (high - low)
    return index, (high - level) * scale, (level - low) * scale


def search_kernel(req, arr, hreq, early, ids, edges, marks_out, worst_out, least_out):
    corners, rows = req.shape
    combos = 2 * corners
    halves = 8 // combos
    depth = halves * HALF
    tables = make_tables(edges)

    def block(step, smallest):
        slabs, parts, spans = [], [], []
        for half in range(halves):
            at = pl.ds(pl.multiple_of(step * depth + half * HALF, HALF), HALF)
            setup = req[:, at] - arr[:, at]
            hold = early[:, at] - hreq[:, at]
            worst_out[0:1, at] = jnp.min(setup, axis=0, keepdims=True)
            worst_out[1:2, at] = jnp.min(hold, axis=0, keepdims=True)
            slabs += [setup, hold]
            parts.append(jnp.broadcast_to(ids[:, at], (combos, HALF)))
            spans.append(at)
        slab = jnp.concatenate(slabs, axis=0)
        part = jnp.concatenate(parts, axis=0)
        low_at, code, w_first, w_second = [], [], [], []
        for lane in range(0, HALF, LANES):
            piece = slab[:, lane : lane + LANES]
            smallest = jnp.minimum(smallest, piece)
            index, wa, wb = search(tables, piece)
            low_at.append((index & (LANES - 1)).astype(jnp.float32))
            code.append(((index >> 7) * GROUPS + part[:, lane : lane + LANES]).astype(jnp.float32))
            w_first.append(wa)
            w_second.append(wb)
        marks = [jnp.concatenate(v, axis=1) for v in (low_at, code, w_first, w_second)]
        marks.append(jnp.minimum(slab, 0.0))
        for q, v in enumerate(marks):
            for half in range(halves):
                marks_out[q, :, spans[half]] = v[half * combos : (half + 1) * combos]
        return smallest

    start = jnp.full((8, LANES), jnp.inf, jnp.float32)
    smallest = lax.fori_loop(0, rows // depth, block, start)
    least_out[...] = jnp.broadcast_to(jnp.min(smallest, axis=1, keepdims=True), (8, LANES))


def report_kernel(
    n, nc, density,
    marks, worst, least, hist_out, stats_out, worst_out,
    acc, hist, hist_in, stats, stats_in, worst_in,
    hs, hr, gs, gr, ss, sr, ws, wr, vs, vr,
):
    combos, rows = marks.shape[1:]
    me = lax.axis_index("ep")
    mc = lax.axis_index("corner")
    chunk = GROUPS // n
    width = worst.shape[1] // nc
    narrow = jnp.bfloat16
    barrier = pltpu.get_barrier_semaphore()
    for d in range(1, n):
        pl.semaphore_signal(
            barrier, inc=1, device_id={"ep": lax.rem(me + d, n)}, device_id_type=MESH
        )
    for d in range(1, nc):
        pl.semaphore_signal(
            barrier, inc=1, device_id={"corner": lax.rem(mc + d, nc)}, device_id_type=MESH
        )
    pl.semaphore_wait(barrier, n - 1 + nc - 1)

    def send(src, dst, s_sem, r_sem, target):
        copy = pltpu.make_async_remote_copy(
            src_ref=src, dst_ref=dst, send_sem=s_sem, recv_sem=r_sem,
            device_id=target, device_id_type=MESH,
        )
        copy.start()
        return copy

    def lanes(k):
        return pl.ds(pl.multiple_of(k * width, LANES), width)

    mins = []
    for d in range(1, nc):
        t = lax.rem(mc + d, nc)
        mins.append(
            send(worst.at[:, lanes(t)], worst_in.at[d], ws.at[d], wr.at[d], {"corner": t})
        )

    iota_low = lax.broadcasted_iota(jnp.int32, (16, DEPTH), 0).astype(jnp.float32).astype(narrow)
    zero = jnp.zeros((16, DEPTH), narrow)
    one = jnp.ones((16, DEPTH), narrow)

    def product(r, first, last):
        def block(step, carry):
            at = pl.ds(pl.multiple_of(step * DEPTH, DEPTH), DEPTH)

            def row(q):
                return marks[q, r : r + 1, at]

            def spread(v):
                return jnp.broadcast_to(v, (16, DEPTH)).astype(narrow)

            at_low, at_code, wa, wb = (spread(row(q)) for q in range(4))
            neg = row(4)
            piece_a = neg.astype(narrow).astype(jnp.float32)
            rest = neg - piece_a
            piece_b = rest.astype(narrow).astype(jnp.float32)
            piece_c = rest - piece_b
            left = []
            for start in range(0, LANES, 16):
                left.append(
                    jnp.where(
                        at_low == iota_low + narrow(start),
                        wa,
                        jnp.where(at_low == iota_low + narrow(start - 1), wb, zero),
                    )
                )
            tail = jnp.where(at_low == narrow(LANES - 1), wb, zero)
            tail = jnp.where(iota_low == narrow(0), tail, zero)
            for place, v in ((1, piece_a), (2, piece_b), (3, piece_c)):
                tail = jnp.where(iota_low == narrow(place), spread(v), tail)
            left.append(jnp.where(iota_low == narrow(4), one, tail))
            right = [
                jnp.where(at_code == iota_low + narrow(start), one, zero)
                for start in range(0, HIGH * GROUPS, 16)
            ]
            acc[...] += lax.dot_general(
                jnp.concatenate(left, axis=0),
                jnp.concatenate(right, axis=0),
                (((1,), (1,)), ((), ())),
                preferred_element_type=jnp.float32,
            )
            return carry

        lax.fori_loop(first, last, block, 0)

    lane = lax.broadcasted_iota(jnp.int32, (1, HIGH * GROUPS), 1)

    def fold(v):
        v = v[:, :LANES] + v[:, LANES:]
        return v + pltpu.roll(jnp.broadcast_to(v, (8, LANES)), GROUPS, 1)[0:1]

    def settle(r):
        full = acc[...]
        over = jnp.broadcast_to(full[LANES : LANES + 1], (8, HIGH * GROUPS))
        over = pltpu.roll(over, GROUPS, 1)[0:1]
        acc[0:1] = full[0:1] + jnp.where(lane >= GROUPS, over, 0.0)
        turned = acc[0:LANES].T
        for k in range(n):
            for g in range(HIGH):
                top = g * GROUPS + k * chunk
                hist[r, k, :, g * LANES : (g + 1) * LANES] = turned[top : top + chunk]
        pieces = [full[LANES + 1 + i : LANES + 2 + i] for i in range(3)]
        stats[r : r + 1] = fold(pieces[0] + pieces[1] + pieces[2])
        if r == 0:
            stats[combos : combos + 1] = fold(full[LANES + 4 : LANES + 5])

    def scatter(r):
        copies = []
        for d in range(1, n):
            t = lax.rem(me + d, n)
            copies.append(
                send(hist.at[r, t], hist_in.at[r, d], hs.at[r, d], hr.at[r, d], {"ep": t})
            )
        return copies

    def gather(r, scattered):
        total = hist[r, me]
        for d in range(1, n):
            scattered[d - 1].wait_recv()
            total += hist_in[r, d]
        hist_out[r, me] = total * density
        copies = []
        for d in range(1, n):
            t = lax.rem(me + d, n)
            part = hist_out.at[r, me]
            copies.append(send(part, part, gs.at[r, d], gr.at[r, d], {"ep": t}))
        return copies

    steps = rows // DEPTH
    stats[...] = jnp.zeros_like(stats)
    stats[8:16] = least[...]
    sent, spread_out, gathered = [], [], []
    for r in range(combos):
        acc[...] = jnp.zeros_like(acc)
        product(r, 0, steps // 2)
        if r == 0:
            for copy in mins:
                copy.wait_recv()
            low = worst[:, lanes(mc)]
            for d in range(1, nc):
                low = jnp.minimum(low, worst_in[d])
            worst_out[:, lanes(mc)] = low
            for d in range(1, nc):
                t = lax.rem(mc + d, nc)
                part = worst_out.at[:, lanes(mc)]
                spread_out.append(send(part, part, vs.at[d], vr.at[d], {"corner": t}))
        else:
            gathered += gather(r - 1, sent[-1])
        product(r, steps // 2, steps)
        settle(r)
        sent.append(scatter(r))
    shares = []
    for d in range(1, n):
        t = lax.rem(me + d, n)
        shares.append(send(stats, stats_in.at[me], ss.at[d], sr.at[d], {"ep": t}))
    gathered += gather(combos - 1, sent[-1])
    for copy in shares:
        copy.wait_recv()
    stats_in[me] = stats[...]
    added = stats_in[0, 0:8]
    lowest = stats_in[0, 8:16]
    for k in range(1, n):
        added += stats_in[k, 0:8]
        lowest = jnp.minimum(lowest, stats_in[k, 8:16])
    stats_out[0:8] = added
    stats_out[8:16] = lowest
    for copy in spread_out + gathered:
        copy.wait_recv()
    for copy in mins + sum(sent, []) + shares + spread_out + gathered:
        copy.wait_send()


def finish_kernel(endpoints, hist, stats, worst, hist_out, tns_out, share_out, total_out, least_out, worst_out):
    corners = total_out.shape[0]
    combos = 2 * corners
    share = GROUPS / endpoints
    for m in range(2):
        for c in range(corners):
            r = m * corners + c
            hist_out[:, c, m, :] = hist[r]
            row = stats[r : r + 1, :GROUPS]
            tns_out[c, m : m + 1, :] = row * share
            total = jnp.sum(row, axis=1, keepdims=True) * (1.0 / endpoints)
            total_out[c : c + 1, m : m + 1] = total
            low = stats[8 + r : 9 + r, 0:1]
            for top in range(8 + combos, 16, combos):
                low = jnp.minimum(low, stats[top + r : top + r + 1, 0:1])
            least_out[c : c + 1, m : m + 1] = low
    share_out[...] = stats[combos : combos + 1, :GROUPS] * share
    worst_out[...] = worst[...]


def on_device(required, arrival, hold_required, early_arrival, part_ids, bin_edges):
    corners, rows = required.shape
    n, nc = lax.axis_size("ep"), lax.axis_size("corner")
    endpoints = rows * n
    bins = bin_edges.shape[0]
    combos = 2 * corners
    f32 = jnp.float32
    vmem = pl.BlockSpec(memory_space=pltpu.VMEM)
    marks, worst, least = pl.pallas_call(
        search_kernel,
        out_shape=(
            jax.ShapeDtypeStruct((5, combos, rows), f32),
            jax.ShapeDtypeStruct((2, rows), f32),
            jax.ShapeDtypeStruct((8, LANES), f32),
        ),
        in_specs=[vmem] * 6,
        out_specs=[vmem] * 3,
        name="node_search",
    )(
        required, arrival, hold_required, early_arrival,
        part_ids.reshape(1, rows), bin_edges.reshape(bins // LANES, LANES),
    )
    dma = pltpu.SemaphoreType.DMA
    blocks = (combos, n, GROUPS // n, bins)
    hist, stats, worst = pl.pallas_call(
        functools.partial(report_kernel, n, nc, GROUPS * bins / endpoints),
        out_shape=(
            jax.ShapeDtypeStruct(blocks, f32),
            jax.ShapeDtypeStruct((16, LANES), f32),
            jax.ShapeDtypeStruct((2, rows), f32),
        ),
        in_specs=[vmem] * 3,
        out_specs=[vmem] * 3,
        scratch_shapes=[
            pltpu.VMEM((LANES + EXTRA, HIGH * GROUPS), f32),
            pltpu.VMEM(blocks, f32),
            pltpu.VMEM(blocks, f32),
            pltpu.VMEM((16, LANES), f32),
            pltpu.VMEM((n, 16, LANES), f32),
            pltpu.VMEM((nc, 2, rows // nc), f32),
        ]
        + [dma((combos, n))] * 4
        + [dma((n,))] * 2
        + [dma((nc,))] * 4,
        compiler_params=pltpu.CompilerParams(collective_id=0, has_side_effects=True),
        name="report",
    )(marks, worst, least)
    part_hist, part_tns, part_share, tns, wns, worst = pl.pallas_call(
        functools.partial(finish_kernel, endpoints),
        out_shape=(
            jax.ShapeDtypeStruct((GROUPS, corners, 2, bins), f32),
            jax.ShapeDtypeStruct((corners, 2, GROUPS), f32),
            jax.ShapeDtypeStruct((1, GROUPS), f32),
            jax.ShapeDtypeStruct((corners, 2), f32),
            jax.ShapeDtypeStruct((corners, 2), f32),
            jax.ShapeDtypeStruct((2, rows), f32),
        ),
        in_specs=[vmem] * 3,
        out_specs=[vmem] * 6,
        name="finish",
    )(hist.reshape(combos, GROUPS, bins), stats, worst)
    return (part_hist, part_tns.transpose(2, 0, 1), part_share[0], tns, wns, worst)


def solution(mesh):
    in_specs = (
        P("corner", "ep"),
        P("corner", "ep"),
        P("corner", "ep"),
        P("corner", "ep"),
        P("ep"),
        P(),
    )
    out_specs = (
        P(None, "corner", None, None),
        P(None, "corner", None),
        P(),
        P("corner", None),
        P("corner", None),
        P(None, "ep"),
    )
    return jax.shard_map(
        on_device, mesh=mesh, in_specs=in_specs, out_specs=out_specs, check_vma=False
    )
```
